32 devices in a mesh: rep: 4 (over z), tp: 8 (over y, x, core).
Axes of the slice: x: 2, y: 2, z: 4, core: 2. Of those that a mesh axis runs over, the one named last changes fastest.
Arguments:
- attn: bfloat16 [3072, 4096], P('rep', 'tp'), parts along dimension 0, may hold values from -6 to 6
- output_weight: bfloat16 [4096, 8192], P(None, 'tp'), may hold values from -0.09375 to 0.09375
- adapter_down_weight: bfloat16 [8, 64, 4096], P('tp'), may hold values from -0.09375 to 0.09375
- adapter_up_weight: bfloat16 [8, 64, 8192], P('tp'), may hold values from -0.75 to 0.75
- block_adapter_index: int32 [24], P('rep'), parts along dimension 0, may hold values from 0 to 7
- adapter_page_table: int32 [8], replicated, may hold values from 0 to 7, each once
Outputs:
- projected: bfloat16 [3072, 8192], P('rep', 'tp'), parts along dimension 0
The draws below stay inside these ranges and needn't reach their ends.
There are 4 independent parts, one for each index of `rep`. The reference program is written for one: setup_inputs(seed, part) draws one part's arguments, and reference() takes and returns one part's arrays. A program takes and returns all parts, laid end to end along the dimension named above; an argument that names none is the same for every part. Nothing has to cross between parts.
Inputs may be any that keep to these rules, and one draw needn't show every extreme that they name: adapter_page_table is a permutation; adapter a is stored on tp device adapter_page_table[a] (each device holds exactly one adapter), and row adapter_page_table[a] of adapter_down_weight and adapter_up_weight holds it. `block_adapter_index`: the adapter used by all 128 tokens of a block.
All inputs are finite; a program needn't handle non-finite values.
Results may differ from the reference program's by a relative error of at most 0.0046.
Values may be sent and summed in bfloat16 or wider, within the bound.
A program may use at most 64 MiB of HBM per device.

```python
import jax
import jax.numpy as jnp
from jax import lax

MODEL_WIDTH = 8192
ADAPTER_RANK = 64
BLOCK = 128
TOKENS = 768
ATTN_FEATURES = 4096
ADAPTER_COUNT = 8
BLOCKS = 6


def place_ends(array, own_key, least, high):
    index_at = [jax.random.randint(jax.random.fold_in(own_key, axis), (), 0, length) for axis, length in enumerate(array.shape)]
    longest = array.shape.index(max(array.shape))
    neighbour = index_at[:longest] + [(index_at[longest] + 1) % array.shape[longest]] + index_at[longest + 1:]
    return array.at[tuple(index_at)].set(least).at[tuple(neighbour)].set(high)


def levels(own_key, extent, shards, smallest, high):
    gain, own = 1.0, jax.random.fold_in(own_key, 6)
    for position, blocks in shards:
        steps = jnp.exp(jax.random.uniform(jax.random.fold_in(own, position), (blocks,), jnp.float32, smallest / len(shards), high / len(shards)))
        gain = gain * jnp.repeat(steps, extent[position] // blocks).reshape([-1 if axis == position else 1 for axis in range(len(extent))])
    return gain


def noise(own_key, shape, deviation, reach, cuts=(), held_as=jnp.bfloat16):
    drawn = jax.random.normal(own_key, shape, jnp.float32) * deviation
    if len(cuts) > 0:
        drawn = levels(own_key, shape, cuts, -0.22, 0.18) * drawn
    return jnp.clip(drawn, min=-reach, max=reach).astype(held_as)


def setup_inputs(seed: int = 0, part: int = 0) -> dict:
    key_list = jax.random.split(jax.random.key(seed), 7)
    own_keys = jax.random.split(jax.random.fold_in(key_list[6], part), 7)
    attn = noise(own_keys[0], (TOKENS, ATTN_FEATURES), 1.0, 6.0, ((1, 8),))
    output_weight = noise(key_list[1], (ATTN_FEATURES, MODEL_WIDTH), ATTN_FEATURES ** -0.5, 0.09375, ((1, 8),))
    adapter_down_weight = noise(key_list[2], (ADAPTER_COUNT, ADAPTER_RANK, ATTN_FEATURES), ATTN_FEATURES ** -0.5, 0.09375, ((0, 8),))
    adapter_up_weight = noise(key_list[3], (ADAPTER_COUNT, ADAPTER_RANK, MODEL_WIDTH), ADAPTER_RANK ** -0.5, 0.75, ((0, 8),))
    block_adapter_index = place_ends(jax.random.randint(own_keys[4], (BLOCKS,), 0, ADAPTER_COUNT), jax.random.fold_in(own_keys[4], 1), 0, ADAPTER_COUNT - 1).astype(jnp.int32)
    adapter_page_table = jax.random.permutation(key_list[5], ADAPTER_COUNT).astype(jnp.int32)
    return {"attn": attn, "output_weight": output_weight, "adapter_down_weight": adapter_down_weight, "adapter_up_weight": adapter_up_weight, "block_adapter_index": block_adapter_index, "adapter_page_table": adapter_page_table}


adapter_scale = 2.0


def reference(attn, output_weight, adapter_down_weight, adapter_up_weight, block_adapter_index, adapter_page_table):
    block_page_index = adapter_page_table[block_adapter_index].astype(jnp.int32)
    base_output = jnp.dot(attn, output_weight, preferred_element_type=jnp.float32)
    row_blocks = attn.reshape(BLOCKS, BLOCK, ATTN_FEATURES).astype(jnp.float32)
    down_block_rows = adapter_down_weight[block_page_index].astype(jnp.float32)
    shrunk = jnp.einsum("btf,brf->brt", row_blocks, down_block_rows, precision=lax.Precision.HIGHEST)
    shrunk_low = lax.optimization_barrier(shrunk.astype(jnp.bfloat16))
    up_block_rows = adapter_up_weight[block_page_index].astype(jnp.float32)
    adapter_output = jnp.einsum("brt,brc->btc", shrunk_low.astype(jnp.float32), up_block_rows, precision=lax.Precision.HIGHEST)
    adapter_output = adapter_output.reshape(TOKENS, MODEL_WIDTH)
    return (base_output + adapter_scale * adapter_output).astype(jnp.bfloat16)
```

```python
import functools

import jax
import jax.numpy as jnp
from jax import lax
from jax.experimental import pallas as pl
from jax.experimental.pallas import tpu as pltpu
from jax.sharding import PartitionSpec as P

adapter_scale = 2.0
MESH = pl.DeviceIdType.MESH


def plain_shards(
    attn,
    output_weight,
    adapter_down_weight,
    adapter_up_weight,
    block_adapter_index,
    adapter_page_table,
):
    tokens = attn.shape[0]
    blocks = block_adapter_index.shape[0]
    block_rows = tokens // blocks
    page_slot_count = adapter_down_weight.shape[0]
    width_out = output_weight.shape[1]
    position = lax.axis_index("tp")
    block_page_index = adapter_page_table[block_adapter_index]
    up_weight_columns = lax.all_to_all(
        adapter_up_weight, "tp", split_axis=2, concat_axis=0, tiled=True
    )
    block_up = up_weight_columns[block_page_index]
    gathered = lax.all_gather(attn, "tp", axis=1, tiled=True)
    base_output = jnp.dot(gathered, output_weight, preferred_element_type=jnp.float32)
    row_blocks = gathered.reshape(blocks, block_rows, gathered.shape[1])
    side_sum = jnp.einsum(
        "btf,srf->bsrt", row_blocks, adapter_down_weight, preferred_element_type=jnp.float32
    )
    own_pages = position * page_slot_count + jnp.arange(page_slot_count, dtype=jnp.int32)
    owned = (block_page_index[:, None] == own_pages[None, :]).astype(jnp.float32)
    local_term = jnp.sum(owned[:, :, None, None] * side_sum, axis=1)
    shrunk = lax.psum(local_term.astype(jnp.bfloat16), "tp")
    adapter_output = jnp.einsum(
        "brt,brc->btc", shrunk, block_up, preferred_element_type=jnp.float32
    )
    adapter_output = adapter_output.reshape(tokens, width_out)
    return (base_output + adapter_scale * adapter_output).astype(jnp.bfloat16)


def kernel(
    n,
    reps,
    index_ref,
    table_ref,
    attn_ref,
    weight_ref,
    down_ref,
    up_ref,
    out_ref,
    a_all,
    w_all,
    acc,
    out_stage,
    dn_all,
    up_all,
    part,
    part_in,
    sum_all,
    send_sem,
    recv_sem,
    local_sem,
):
    blocks = index_ref.shape[0]
    rows = a_all.shape[1] // blocks
    rank = dn_all.shape[1]
    f_own = a_all.shape[2]
    c_own = up_all.shape[2]
    share = rank // reps
    red = rank // n
    me = lax.axis_index("tp")
    z = lax.axis_index("rep")
    core = lax.rem(me, 2)
    x_at = lax.rem(me // 2, 2)
    y_at = me // 4
    mate = me + 1 - 2 * core
    xn = me + 2 - 4 * x_at
    yn = me + 4 - 8 * y_at
    dg = xn + 4 - 8 * y_at

    def mate_of(d):
        return d + 1 - 2 * core

    counts = [0, 0]
    sends = []

    def remote(src, dst, axis, target):
        k = counts[0]
        counts[0] += 1
        copy = pltpu.make_async_remote_copy(
            src_ref=src,
            dst_ref=dst,
            send_sem=send_sem.at[k],
            recv_sem=recv_sem.at[k],
            device_id={axis: target},
            device_id_type=MESH,
        )
        copy.start()
        sends.append(copy)
        return copy

    def local(src, dst):
        k = counts[1]
        counts[1] += 1
        copy = pltpu.make_async_copy(src, dst, local_sem.at[k])
        copy.start()
        return copy

    own_load = local(attn_ref, a_all.at[me])
    z_rows = pl.ds(pl.multiple_of(z * share, share), share)
    own_f = pl.ds(pl.multiple_of(me * f_own, f_own), f_own)
    own_c = pl.ds(pl.multiple_of(me * c_own, c_own), c_own)
    own_dn = local(down_ref.at[0, z_rows, own_f], dn_all.at[me, z_rows, :])
    own_up = local(up_ref.at[0, z_rows, own_c], up_all.at[me, z_rows, :])

    barrier = pltpu.get_barrier_semaphore()
    for d in range(1, n):
        pl.semaphore_signal(
            barrier, inc=1, device_id={"tp": lax.rem(me + d, n)}, device_id_type=MESH
        )
    for d in range(1, reps):
        pl.semaphore_signal(
            barrier, inc=1, device_id={"rep": lax.rem(z + d, reps)}, device_id_type=MESH
        )
    pl.semaphore_wait(barrier, n - 1 + reps - 1)

    dn_copies, up_copies = [], []
    for d in range(1, n):
        j = lax.rem(me + d, n)
        cols = pl.ds(pl.multiple_of(j * f_own, f_own), f_own)
        dn_copies.append(
            remote(down_ref.at[0, z_rows, cols], dn_all.at[me, z_rows, :], "tp", j)
        )
    for d in range(1, n):
        j = lax.rem(me + d, n)
        cols = pl.ds(pl.multiple_of(j * c_own, c_own), c_own)
        up_copies.append(
            remote(up_ref.at[0, z_rows, cols], up_all.at[me, z_rows, :], "tp", j)
        )

    own_load.wait()

    def chunk(slot, b):
        return a_all.at[slot, pl.ds(b * rows, rows), :]

    x_copies = []
    y_copies = []
    mate_copy = remote(a_all.at[me], a_all.at[me], "tp", mate)
    for b in range(blocks):
        x_copies.append(remote(chunk(me, b), chunk(me, b), "tp", xn))
        y_copies.append(remote(chunk(me, b), chunk(me, b), "tp", yn))

    w_loads = [local(weight_ref.at[pl.ds(pl.multiple_of(s * f_own, f_own), f_own), :], w_all.at[s])
               for s in (me, mate, xn, mate_of(xn), yn, mate_of(yn), dg, mate_of(dg))]

    own_dn.wait()
    for copy in dn_copies:
        copy.wait_recv()
    dn_z = [
        remote(dn_all.at[:, z_rows, :], dn_all.at[:, z_rows, :], "rep", lax.rem(z + d, reps))
        for d in range(1, reps)
    ]
    own_up.wait()
    for copy in up_copies:
        copy.wait_recv()
    up_z = [
        remote(up_all.at[:, z_rows, :], up_all.at[:, z_rows, :], "rep", lax.rem(z + d, reps))
        for d in range(1, reps)
    ]

    width = acc.shape[1]
    tile = 256

    def multiply(first, size, slots, fresh):
        at = pl.ds(first, size)

        @pl.loop(0, width // tile)
        def _(t):
            cols = pl.ds(pl.multiple_of(t * tile, tile), tile)
            total = None
            for s in slots:
                term = jnp.dot(
                    a_all[s, at, :], w_all[s, :, cols], preferred_element_type=jnp.float32
                )
                total = term if total is None else total + term
            if fresh:
                acc[at, cols] = total
            else:
                acc[at, cols] += total

    pair = 2 * rows
    mate_copy.wait_recv()
    w_loads[0].wait()
    w_loads[1].wait()
    for s in range(blocks // 2):
        multiply(s * pair, pair, (me, mate), True)

    def pages(b):
        return table_ref[index_ref[b]]

    def shrink():
        for copy in dn_z:
            copy.wait_recv()
        for b in range(blocks):
            part[b] = lax.dot_general(
                dn_all[pages(b)],
                a_all[me, pl.ds(b * rows, rows), :],
                (((1,), (1,)), ((), ())),
                preferred_element_type=jnp.float32,
            )
        copies = []
        for d in range(1, n):
            j = lax.rem(me + d, n)
            copies.append(
                remote(
                    part.at[:, pl.ds(pl.multiple_of(j * red, red), red), :],
                    part_in.at[d - 1],
                    "tp",
                    j,
                )
            )
        return copies

    def reduce(copies):
        mine = pl.ds(pl.multiple_of(me * red, red), red)
        total = part[:, mine, :]
        for d in range(1, n):
            copies[d - 1].wait_recv()
            total = total + part_in[d - 1]
        sum_all[:, mine, :] = total
        return [
            remote(sum_all.at[:, mine, :], sum_all.at[:, mine, :], "tp", lax.rem(me + d, n))
            for d in range(1, n)
        ]

    x_mate, y_mate, dg_copies = [], [], []
    for s in range(blocks // 2):
        for b in (2 * s, 2 * s + 1):
            x_copies[b].wait_recv()
            if b % 2 == 1:
                dg_copies.append(remote(chunk(xn, b), chunk(xn, b), "tp", yn))
            x_mate.append(remote(chunk(xn, b), chunk(xn, b), "tp", mate))
            y_copies[b].wait_recv()
            if b % 2 == 0:
                dg_copies.append(remote(chunk(yn, b), chunk(yn, b), "tp", xn))
            y_mate.append(remote(chunk(yn, b), chunk(yn, b), "tp", mate))
        if s == 0:
            for load in w_loads[2:6]:
                load.wait()
        x_mate[2 * s].wait_recv()
        x_mate[2 * s + 1].wait_recv()
        y_mate[2 * s].wait_recv()
        y_mate[2 * s + 1].wait_recv()
        multiply(s * pair, pair, (xn, mate_of(xn), yn, mate_of(yn)), False)
        if s == blocks // 2 - 2:
            part_copies = shrink()
    sum_copies = reduce(part_copies)

    w_loads[6].wait()
    w_loads[7].wait()
    dg_mate = []
    out_copies = []
    for s in range(blocks // 2):
        for b in (2 * s, 2 * s + 1):
            dg_copies[b].wait_recv()
            dg_mate.append(remote(chunk(dg, b), chunk(dg, b), "tp", mate))
        if s == 0:
            for copy in sum_copies:
                copy.wait_recv()
            for copy in up_z:
                copy.wait_recv()
        for b in (2 * s, 2 * s + 1):
            low = sum_all[b].astype(jnp.bfloat16)
            page = pages(b)
            at = pl.ds(b * rows, rows)
            adapted = lax.dot_general(
                low, up_all[page], (((0,), (0,)), ((), ())), preferred_element_type=jnp.float32
            )
            acc[at, :] += adapter_scale * adapted
        dg_mate[2 * s].wait_recv()
        dg_mate[2 * s + 1].wait_recv()
        at = pl.ds(s * pair, pair)

        @pl.loop(0, width // tile)
        def _(t):
            cols = pl.ds(pl.multiple_of(t * tile, tile), tile)
            total = acc[at, cols]
            for slot in (dg, mate_of(dg)):
                total = total + jnp.dot(
                    a_all[slot, at, :], w_all[slot, :, cols], preferred_element_type=jnp.float32
                )
            out_stage[at, cols] = total.astype(out_stage.dtype)

        out_copies.append(local(out_stage.at[at, :], out_ref.at[at, :]))

    for copy in sends:
        copy.wait_send()
    for copy in out_copies:
        copy.wait()


def shards(n, reps, attn, weight, down, up, index, table):
    tokens, f_own = attn.shape
    blocks = index.shape[0]
    rows = tokens // blocks
    features, width = weight.shape
    rank = down.shape[1]
    copies = 2 * (n - 1) + 1 + 2 * blocks + 2 * (reps - 1) + 4 * blocks + 2 * (n - 1)
    return pl.pallas_call(
        functools.partial(kernel, n, reps),
        out_shape=jax.ShapeDtypeStruct((tokens, width), jnp.bfloat16),
        in_specs=[pl.BlockSpec(memory_space=pltpu.SMEM)] * 2
        + [pl.BlockSpec(memory_space=pl.ANY)] * 4,
        out_specs=pl.BlockSpec(memory_space=pl.ANY),
        scratch_shapes=[
            pltpu.VMEM((n, tokens, f_own), jnp.bfloat16),
            pltpu.VMEM((n, features // n, width), jnp.bfloat16),
            pltpu.VMEM((tokens, width), jnp.float32),
            pltpu.VMEM((tokens, width), jnp.bfloat16),
            pltpu.VMEM((n, rank, f_own), jnp.bfloat16),
            pltpu.VMEM((n, rank, width), jnp.bfloat16),
            pltpu.VMEM((blocks, rank, rows), jnp.float32),
            pltpu.VMEM((n - 1, blocks, rank // n, rows), jnp.float32),
            pltpu.VMEM((blocks, rank, rows), jnp.float32),
            pltpu.SemaphoreType.DMA((copies,)),
            pltpu.SemaphoreType.DMA((copies,)),
            pltpu.SemaphoreType.DMA((3 + n + blocks // 2,)),
        ],
        compiler_params=pltpu.CompilerParams(
            collective_id=0, has_side_effects=True, vmem_limit_bytes=60 * 1024 * 1024
        ),
    )(index, table, attn, weight, down, up)


def solution(mesh):
    n, reps = mesh.shape["tp"], mesh.shape["rep"]

    def body(attn, weight, down, up, index, table):
        blocks = index.shape[0]
        fits = (
            n == 8
            and reps > 1
            and blocks % 2 == 0
            and blocks >= 4
            and down.shape[0] == 1
            and down.shape[1] % (16 * reps) == 0
            and down.shape[1] % (8 * n) == 0
            and attn.shape[0] % (128 * blocks) == 0
            and attn.shape[1] % 128 == 0
            and weight.shape[1] % 256 == 0
        )
        if fits:
            return shards(n, reps, attn, weight, down, up, index, table)
        return plain_shards(attn, weight, down, up, index, table)

    return jax.shard_map(
        body,
        mesh=mesh,
        in_specs=(
            P("rep", "tp"),
            P(None, "tp"),
            P("tp", None, None),
            P("tp", None, None),
            P("rep"),
            P(),
        ),
        out_specs=P("rep", "tp"),
        check_vma=False,
    )
```

```python
import functools

import jax
import jax.numpy as jnp
from jax import lax
from jax.experimental import pallas as pl
from jax.experimental.pallas import tpu as pltpu
from jax.sharding import PartitionSpec as P

adapter_scale = 2.0
MESH = pl.DeviceIdType.MESH


def plain_shards(
    attn,
    output_weight,
    adapter_down_weight,
    adapter_up_weight,
    block_adapter_index,
    adapter_page_table,
):
    tokens = attn.shape[0]
    blocks = block_adapter_index.shape[0]
    block_rows = tokens // blocks
    page_slot_count = adapter_down_weight.shape[0]
    width_out = output_weight.shape[1]
    position = lax.axis_index("tp")
    block_page_index = adapter_page_table[block_adapter_index]
    up_weight_columns = lax.all_to_all(
        adapter_up_weight, "tp", split_axis=2, concat_axis=0, tiled=True
    )
    block_up = up_weight_columns[block_page_index]
    gathered = lax.all_gather(attn, "tp", axis=1, tiled=True)
    base_output = jnp.dot(gathered, output_weight, preferred_element_type=jnp.float32)
    row_blocks = gathered.reshape(blocks, block_rows, gathered.shape[1])
    side_sum = jnp.einsum(
        "btf,srf->bsrt", row_blocks, adapter_down_weight, preferred_element_type=jnp.float32
    )
    own_pages = position * page_slot_count + jnp.arange(page_slot_count, dtype=jnp.int32)
    owned = (block_page_index[:, None] == own_pages[None, :]).astype(jnp.float32)
    local_term = jnp.sum(owned[:, :, None, None] * side_sum, axis=1)
    shrunk = lax.psum(local_term.astype(jnp.bfloat16), "tp")
    adapter_output = jnp.einsum(
        "brt,brc->btc", shrunk, block_up, preferred_element_type=jnp.float32
    )
    adapter_output = adapter_output.reshape(tokens, width_out)
    return (base_output + adapter_scale * adapter_output).astype(jnp.bfloat16)


depth = 3


def link_orders(blocks):
    x_order, y_order = [(False, 1), (False, 0), (False, 3)], [(False, 0), (False, 1), (False, 2)]
    for s in range(blocks // 2):
        x_order.append((True, 2 * s))
        y_order.append((True, 2 * s + 1))
        for order, b in ((x_order, 2 * s + 2), (x_order, 2 * s + 5), (y_order, 2 * s + 3), (y_order, 2 * s + 4)):
            if b < blocks:
                order.append((False, b))
    return x_order, y_order


def kernel(
    n,
    reps,
    index_ref,
    table_ref,
    attn_ref,
    weight_ref,
    down_ref,
    up_ref,
    out_ref,
    a_all,
    w_all,
    acc,
    out_stage,
    dn_all,
    up_all,
    part,
    half_in,
    chip_part,
    part_in,
    sum_all,
    send_sem,
    recv_sem,
    local_sem,
):
    blocks = index_ref.shape[0]
    rows = a_all.shape[1] // blocks
    rank = dn_all.shape[1]
    f_own = a_all.shape[2]
    c_own = up_all.shape[2]
    share = rank // reps
    red = rank // n
    me = lax.axis_index("tp")
    z = lax.axis_index("rep")
    core = lax.rem(me, 2)
    x_at = lax.rem(me // 2, 2)
    y_at = me // 4
    mate = me + 1 - 2 * core
    xn = me + 2 - 4 * x_at
    yn = me + 4 - 8 * y_at
    dg = xn + 4 - 8 * y_at

    def mate_of(d):
        return d + 1 - 2 * core

    counts = [0, 0]
    sends = []

    def remote(src, dst, axis, target):
        k = counts[0]
        counts[0] += 1
        copy = pltpu.make_async_remote_copy(
            src_ref=src,
            dst_ref=dst,
            send_sem=send_sem.at[k],
            recv_sem=recv_sem.at[k],
            device_id={axis: target},
            device_id_type=MESH,
        )
        copy.start()
        sends.append(copy)
        return copy

    def local(src, dst):
        k = counts[1]
        counts[1] += 1
        copy = pltpu.make_async_copy(src, dst, local_sem.at[k])
        copy.start()
        return copy

    own_load = local(attn_ref, a_all.at[me])
    z_rows = pl.ds(pl.multiple_of(z * share, share), share)
    own_f = pl.ds(pl.multiple_of(me * f_own, f_own), f_own)
    own_c = pl.ds(pl.multiple_of(me * c_own, c_own), c_own)
    own_dn = local(down_ref.at[0, :, own_f], dn_all.at[me])
    own_up = local(up_ref.at[0, z_rows, own_c], up_all.at[me, z_rows, :])

    barrier = pltpu.get_barrier_semaphore()
    for d in range(1, n):
        pl.semaphore_signal(
            barrier, inc=1, device_id={"tp": lax.rem(me + d, n)}, device_id_type=MESH
        )
    for d in range(1, reps):
        pl.semaphore_signal(
            barrier, inc=1, device_id={"rep": lax.rem(z + d, reps)}, device_id_type=MESH
        )
    pl.semaphore_wait(barrier, n - 1 + reps - 1)

    dn_copies, up_copies = [], []
    for d in range(1, n):
        j = lax.rem(me + d, n)
        cols = pl.ds(pl.multiple_of(j * f_own, f_own), f_own)
        dn_copies.append(
            remote(down_ref.at[0, :, cols], dn_all.at[me], "tp", j)
        )
    for d in range(1, n):
        j = lax.rem(me + d, n)
        cols = pl.ds(pl.multiple_of(j * c_own, c_own), c_own)
        up_copies.append(
            remote(up_ref.at[0, z_rows, cols], up_all.at[me, z_rows, :], "tp", j)
        )

    own_load.wait()

    def chunk(slot, b):
        return a_all.at[slot, pl.ds(b * rows, rows), :]

    x_order, y_order = link_orders(blocks)
    x_copies, y_copies, x_mate, y_mate = [], [], {}, {}

    def issue(k):
        if k < len(x_order):
            passed, b = x_order[k]
            slot = yn if passed else me
            x_copies.append(remote(chunk(slot, b), chunk(slot, b), "tp", xn))
            passed, b = y_order[k]
            slot = xn if passed else me
            y_copies.append(remote(chunk(slot, b), chunk(slot, b), "tp", yn))

    def event(k):
        x_copies[k].wait_recv()
        y_copies[k].wait_recv()
        issue(k + depth)
        passed, b = x_order[k]
        slot = dg if passed else xn
        x_mate[passed, b] = remote(chunk(slot, b), chunk(slot, b), "tp", mate)
        passed, b = y_order[k]
        slot = dg if passed else yn
        y_mate[passed, b] = remote(chunk(slot, b), chunk(slot, b), "tp", mate)

    issue(0)
    mate_copy = remote(a_all.at[me], a_all.at[me], "tp", mate)
    issue(1)

    w_loads = [local(weight_ref.at[pl.ds(pl.multiple_of(s * f_own, f_own), f_own), :], w_all.at[s])
               for s in (me, mate, xn, mate_of(xn), yn, mate_of(yn), dg, mate_of(dg))]

    width = acc.shape[1]
    tile = 256
    pair = 2 * rows
    pairs = blocks // 2

    def multiply(s, slots, fresh=False):
        at = pl.ds(s * pair, pair)

        @pl.loop(0, width // tile)
        def _(t):
            cols = pl.ds(pl.multiple_of(t * tile, tile), tile)
            total = None if fresh else acc[at, cols]
            for slot in slots:
                term = jnp.dot(
                    a_all[slot, at, :], w_all[slot, :, cols], preferred_element_type=jnp.float32
                )
                total = term if total is None else total + term
            acc[at, cols] = total

    def multiply_sides(s):
        for b in (2 * s, 2 * s + 1):
            x_mate[False, b].wait_recv()
            y_mate[False, b].wait_recv()
        multiply(s, (xn, mate_of(xn), yn, mate_of(yn)))

    def multiply_diagonal(s):
        x_mate[True, 2 * s].wait_recv()
        y_mate[True, 2 * s + 1].wait_recv()
        multiply(s, (dg, mate_of(dg)))

    half = rank // 2
    my_half = pl.ds(pl.multiple_of(core * half, half), half)
    mate_half = pl.ds(pl.multiple_of((1 - core) * half, half), half)

    def piece(device):
        return pl.ds(pl.multiple_of(core * half + (device // 2) * red, red), red)

    peers = (xn, yn, dg)

    def pages(b):
        return table_ref[index_ref[b]]

    own_dn.wait()
    for copy in dn_copies:
        copy.wait_recv()
    for b in range(blocks):
        part[b] = lax.dot_general(
            dn_all[pages(b)],
            a_all[me, pl.ds(b * rows, rows), :],
            (((1,), (1,)), ((), ())),
            preferred_element_type=jnp.float32,
        )
    half_copy = remote(part.at[:, mate_half, :], half_in, "tp", mate)
    mate_copy.wait_recv()
    w_loads[0].wait()
    w_loads[1].wait()
    multiply(0, (me, mate), True)
    half_copy.wait_recv()
    chip_part[:, my_half, :] = part[:, my_half, :] + half_in[...]
    part_copies = [
        remote(chip_part.at[:, piece(p), :], part_in.at[i], "tp", p) for i, p in enumerate(peers)
    ]
    issue(2)
    own_up.wait()
    for copy in up_copies:
        copy.wait_recv()
    up_z = [
        remote(up_all.at[:, z_rows, :], up_all.at[:, z_rows, :], "rep", lax.rem(z + d, reps))
        for d in range(1, reps)
    ]
    event(0)
    multiply(1, (me, mate), True)
    event(1)
    for s in range(2, pairs):
        multiply(s, (me, mate), True)
    for load in w_loads[2:]:
        load.wait()
    event(2)
    total = chip_part[:, piece(me), :]
    for i in range(len(peers)):
        part_copies[i].wait_recv()
        total = total + part_in[i]
    sum_all[:, piece(me), :] = total
    sum_copies = [
        remote(sum_all.at[:, piece(me), :], sum_all.at[:, piece(me), :], "tp", p) for p in peers
    ]
    multiply_sides(0)

    event(3)
    event(4)
    multiply_sides(1)
    event(5)
    multiply_diagonal(0)
    event(6)
    for copy in sum_copies:
        copy.wait_recv()
    sum_mate = remote(sum_all.at[:, my_half, :], sum_all.at[:, my_half, :], "tp", mate)
    multiply_diagonal(1)
    event(7)
    sum_mate.wait_recv()
    for copy in up_z:
        copy.wait_recv()
    for b in range(blocks):
        at = pl.ds(b * rows, rows)
        adapted = lax.dot_general(
            sum_all[b].astype(jnp.bfloat16),
            up_all[pages(b)],
            (((0,), (0,)), ((), ())),
            preferred_element_type=jnp.float32,
        )
        acc[at, :] += adapter_scale * adapted
    multiply_sides(pairs - 1)
    out_copies = []
    for s in range(pairs - 1):
        at = pl.ds(s * pair, pair)
        out_stage[at, :] = acc[at, :].astype(out_stage.dtype)
        out_copies.append(local(out_stage.at[at, :], out_ref.at[at, :]))
    event(8)
    last = pairs - 1
    multiply(last, (dg,))
    x_mate[True, 2 * last].wait_recv()
    y_mate[True, 2 * last + 1].wait_recv()
    at = pl.ds(last * pair, pair)

    @pl.loop(0, width // tile)
    def _(t):
        cols = pl.ds(pl.multiple_of(t * tile, tile), tile)
        slot = mate_of(dg)
        total = acc[at, cols] + jnp.dot(
            a_all[slot, at, :], w_all[slot, :, cols], preferred_element_type=jnp.float32
        )
        out_stage[at, cols] = total.astype(out_stage.dtype)

    out_copies.append(local(out_stage.at[at, :], out_ref.at[at, :]))
    for copy in sends:
        copy.wait_send()
    for copy in out_copies:
        copy.wait()


def shards(n, reps, attn, weight, down, up, index, table):
    tokens, f_own = attn.shape
    blocks = index.shape[0]
    rows = tokens // blocks
    features, width = weight.shape
    rank = down.shape[1]
    copies = 2 * (n - 1) + 1 + 3 * blocks + (reps - 1) + 3 * blocks + 2 * (n // 2 - 1) + 2
    return pl.pallas_call(
        functools.partial(kernel, n, reps),
        out_shape=jax.ShapeDtypeStruct((tokens, width), jnp.bfloat16),
        in_specs=[pl.BlockSpec(memory_space=pltpu.SMEM)] * 2
        + [pl.BlockSpec(memory_space=pl.ANY)] * 4,
        out_specs=pl.BlockSpec(memory_space=pl.ANY),
        scratch_shapes=[
            pltpu.VMEM((n, tokens, f_own), jnp.bfloat16),
            pltpu.VMEM((n, features // n, width), jnp.bfloat16),
            pltpu.VMEM((tokens, width), jnp.float32),
            pltpu.VMEM((tokens, width), jnp.bfloat16),
            pltpu.VMEM((n, rank, f_own), jnp.bfloat16),
            pltpu.VMEM((n, rank, width), jnp.bfloat16),
            pltpu.VMEM((blocks, rank, rows), jnp.float32),
            pltpu.VMEM((blocks, rank // 2, rows), jnp.float32),
            pltpu.VMEM((blocks, rank, rows), jnp.float32),
            pltpu.VMEM((n // 2 - 1, blocks, rank // n, rows), jnp.float32),
            pltpu.VMEM((blocks, rank, rows), jnp.float32),
            pltpu.SemaphoreType.DMA((copies,)),
            pltpu.SemaphoreType.DMA((copies,)),
            pltpu.SemaphoreType.DMA((3 + n + blocks // 2,)),
        ],
        compiler_params=pltpu.CompilerParams(
            collective_id=0, has_side_effects=True, vmem_limit_bytes=60 * 1024 * 1024
        ),
    )(index, table, attn, weight, down, up)


def solution(mesh):
    n, reps = mesh.shape["tp"], mesh.shape["rep"]

    def body(attn, weight, down, up, index, table):
        blocks = index.shape[0]
        fits = (
            n == 8
            and reps > 1
            and blocks % 2 == 0
            and blocks == 6
            and down.shape[0] == 1
            and down.shape[1] % (16 * reps) == 0
            and down.shape[1] % (8 * n) == 0
            and attn.shape[0] % (128 * blocks) == 0
            and attn.shape[1] % 128 == 0
            and weight.shape[1] % 256 == 0
        )
        if fits:
            return shards(n, reps, attn, weight, down, up, index, table)
        return plain_shards(attn, weight, down, up, index, table)

    return jax.shard_map(
        body,
        mesh=mesh,
        in_specs=(
            P("rep", "tp"),
            P(None, "tp"),
            P("tp", None, None),
            P("tp", None, None),
            P("rep"),
            P(),
        ),
        out_specs=P("rep", "tp"),
        check_vma=False,
    )
```
